128 devices in a mesh: rep: 1, dp: 128 (over x, y, z, core).
Axes of the slice: x: 4, y: 4, z: 4, core: 2. Of those that a mesh axis runs over, the one named last changes fastest.
Arguments:
- x: bfloat16 [128, 1024, 1024], P(('rep', 'dp'))
- dy: bfloat16 [128, 1024, 1024], P(('rep', 'dp'))
- wq: bfloat16 [1, 1024, 1024], P(None, 'dp')
- wk: bfloat16 [1, 1024, 1024], P(None, 'dp')
- wv: bfloat16 [1, 1024, 1024], P(None, 'dp')
- wo: bfloat16 [1, 1024, 1024], P(None, 'dp')
- w_gate: bfloat16 [1, 1024, 4096], P(None, 'dp')
- w_up: bfloat16 [1, 1024, 4096], P(None, 'dp')
- w_down: bfloat16 [1, 4096, 1024], P(None, 'dp')
Outputs:
- output 1: bfloat16 [128, 1024, 1024], P(('rep', 'dp'))
- output 2: bfloat16 [1, 1024, 1024], P('rep', 'dp')
- output 3: bfloat16 [1, 1024, 1024], P('rep', 'dp')
- output 4: bfloat16 [1, 1024, 1024], P('rep', 'dp')
- output 5: bfloat16 [1, 1024, 1024], P('rep', 'dp')
- output 6: bfloat16 [1, 1024, 4096], P('rep', 'dp')
- output 7: bfloat16 [1, 1024, 4096], P('rep', 'dp')
- output 8: bfloat16 [1, 4096, 1024], P('rep', 'dp')
All inputs are finite; a program needn't handle non-finite values.
Results may differ from the reference program's by a relative error of at most 0.0293.
Values are sent between devices in bfloat16 or wider.
A program may use at most 1.5 GiB of HBM per device.

```python
import jax
import jax.numpy as jnp
from jax import lax

SEQUENCES = 128
TOKENS = 1024
D = 1024
HEADS = 4
KV_HEADS = 4
HEAD = 256
FF = 4096
LAYERS = 1
THETA = 10000
NAMES = ("wq", "wk", "wv", "wo", "w_gate", "w_up", "w_down")
SHAPES = {
    "wq": (LAYERS, D, HEADS * HEAD),
    "wk": (LAYERS, D, KV_HEADS * HEAD),
    "wv": (LAYERS, D, KV_HEADS * HEAD),
    "wo": (LAYERS, HEADS * HEAD, D),
    "w_gate": (LAYERS, D, FF),
    "w_up": (LAYERS, D, FF),
    "w_down": (LAYERS, FF, D),
}


def bump(key, n, height):
    away = (jnp.arange(n, dtype=jnp.int32) - jax.random.randint(key, (), 0, n, jnp.int32)) % n
    return jnp.where(away < n // 8, height, 1.0)


def together(key, own, strength):
    shared = jax.random.normal(key, own.shape[1:], jnp.float32)
    return (own + strength * shared) * lax.rsqrt(1 + strength * strength)


def setup_inputs(seed: int = 0, part: int = 0) -> dict:
    kx, kdy, ka, kb, kz, kf, kh, kl, *keys = jax.random.split(jax.random.key(seed), 8 + 3 * len(NAMES))
    kx, kdy, ka, kb = (jax.random.fold_in(k, part) for k in (kx, kdy, ka, kb))
    kw, km, kv = (keys[i::3] for i in range(3))
    shape = (SEQUENCES, TOKENS, D)
    much_x, much_dy = jax.random.uniform(kz, (2,), jnp.float32, 0.0, 1.0)
    loud = 2.0 ** jax.random.uniform(jax.random.fold_in(kz, 1), (), jnp.float32, -1.0, 2.0)
    layers = 2.0 ** jax.random.uniform(kl, (LAYERS, 1, 1), jnp.float32, -1.0, 1.0)
    times = {"wq": 1.0, "wk": 1.0, "wv": 2.0, "wo": layers, "w_gate": 1.0, "w_up": bump(kh, FF, 4.0), "w_down": layers}
    x = together(ka, jax.random.normal(kx, shape, jnp.float32), much_x) * bump(kf, D, 4.0)
    dy = together(kb, jax.random.normal(kdy, shape, jnp.float32), much_dy)
    drawn = {"x": x.astype(jnp.bfloat16), "dy": (loud * dy * (SEQUENCES * TOKENS) ** -0.5).astype(jnp.bfloat16)}
    for key, name in zip(kw, NAMES, strict=True):
        drawn[name] = (jax.random.normal(key, SHAPES[name], jnp.float32) * SHAPES[name][1] ** -0.5 * times[name]).astype(jnp.bfloat16)
    return drawn


def matmul(a, w):
    return jnp.dot(a, w, preferred_element_type=jnp.float32).astype(jnp.bfloat16)


def normed(h):
    wide = h.astype(jnp.float32)
    scale = lax.rsqrt(jnp.mean(wide**2, -1, keepdims=True) + 1e-6)
    return (wide * scale).astype(jnp.bfloat16)


def turned(t, theta):
    half = t.shape[-1] // 2
    angle = jnp.arange(t.shape[0], dtype=jnp.float32)[:, None] * theta ** (-jnp.arange(half, dtype=jnp.float32) / half)
    cos, sin = jnp.cos(angle)[:, None], jnp.sin(angle)[:, None]
    a, b = t[..., :half].astype(jnp.float32), t[..., half:].astype(jnp.float32)
    return jnp.concatenate([a * cos - b * sin, b * cos + a * sin], -1).astype(jnp.bfloat16)


def seen_by(q, k, v):
    tokens, kv = q.shape[0], k.shape[1]
    q = q.reshape(tokens, kv, -1, q.shape[-1])
    scores = jnp.einsum("tgsd,ugd->gstu", q.astype(jnp.float32), k.astype(jnp.float32)) * q.shape[-1] ** -0.5
    place = jnp.arange(tokens)
    weights = jax.nn.softmax(jnp.where(place[:, None] >= place, scores, -jnp.inf), -1).astype(jnp.bfloat16)
    return jnp.einsum("gstu,ugd->tgsd", weights.astype(jnp.float32), v.astype(jnp.float32)).astype(jnp.bfloat16).reshape(tokens, -1)


def layer(h, w):
    a = normed(h)
    q, k = (turned(matmul(a, w[name]).reshape(h.shape[0], -1, HEAD), THETA) for name in ("wq", "wk"))
    h = h + matmul(seen_by(q, k, matmul(a, w["wv"]).reshape(h.shape[0], -1, HEAD)), w["wo"])
    b = normed(h)
    gate = jnp.dot(b, w["w_gate"], preferred_element_type=jnp.float32)
    up = jnp.dot(b, w["w_up"], preferred_element_type=jnp.float32)
    return h + matmul((jax.nn.silu(gate) * up).astype(jnp.bfloat16), w["w_down"])


def stack(weights, h):
    return lax.scan(lambda h, w: (layer(h, w), None), h, weights)[0]


def reference(x, dy, wq, wk, wv, wo, w_gate, w_up, w_down):
    weights = dict(zip(NAMES, (wq, wk, wv, wo, w_gate, w_up, w_down), strict=True))

    def take(so_far, sequence):
        h, by_y = sequence
        _, back = jax.vjp(stack, weights, h)
        by_weights, by_h = back(by_y)
        return jax.tree.map(lambda total, term: total + term.astype(jnp.float32), so_far, by_weights), by_h

    none_yet = {name: jnp.zeros(w.shape, jnp.float32) for name, w in weights.items()}
    by_weights, by_x = lax.scan(take, none_yet, (x, dy))
    return (by_x, *(by_weights[name].astype(jnp.bfloat16) for name in NAMES))
```

```python
import functools

import jax
import jax.numpy as jnp
from jax import lax
from jax.experimental import pallas as pl
from jax.experimental.pallas import tpu as pltpu
from jax.sharding import PartitionSpec as P

NAMES = ("wq", "wk", "wv", "wo", "w_gate", "w_up", "w_down")
HEAD, THETA, EPS = 256, 10000, 1e-6
T = D = 1024
FF = 4096
BQ = 256
SCALE = HEAD**-0.5
LOG2E = 1.4426950408889634
bf16, f32 = jnp.bfloat16, jnp.float32


def dot(a, b, ca, cb):
    return lax.dot_general(a, b, (((ca,), (cb,)), ((), ())), preferred_element_type=f32)


def wide(v):
    return v.astype(f32)


def low(v):
    return v.astype(bf16)


def turn(t, cos, sin):
    half = HEAD // 2
    a, b = t[:, :half], t[:, half:]
    return jnp.concatenate([a * cos - b * sin, b * cos + a * sin], axis=1)


def seen(n):
    return lax.broadcasted_iota(jnp.int32, (n, BQ), 1) >= lax.broadcasted_iota(jnp.int32, (n, BQ), 0)


def masked(s, n, fill):
    diagonal = jnp.where(seen(BQ), s[n - BQ :], fill)
    return diagonal if n == BQ else jnp.concatenate([s[: n - BQ], diagonal], axis=0)


def attend_kernel(q_ref, k_ref, v_ref, cos_ref, sin_ref, o_ref, qr_ref, kr_ref, lse_ref):
    cos, sin = cos_ref[...], sin_ref[...]
    qr_ref[...] = low(turn(wide(q_ref[...]), cos, sin))
    kr_ref[...] = low(turn(wide(k_ref[...]), cos, sin))
    for at in range(0, T, BQ):
        n, mine = at + BQ, slice(at, at + BQ)
        s = masked(dot(kr_ref[:n, :], qr_ref[mine, :], 1, 1), n, -1e30)
        top = s.max(axis=0, keepdims=True)
        p = jnp.exp2((s - top) * (SCALE * LOG2E))
        total = p.sum(axis=0, keepdims=True)
        o_ref[mine, :] = low((dot(v_ref[:n, :], low(p), 0, 0) * (1 / total)).T)
        lse_ref[0, :, mine] = top * (SCALE * LOG2E) + jnp.log2(total)


def attend_back_kernel(qr_ref, kr_ref, v_ref, o_ref, do_ref, lse_ref, cos_ref, sin_ref, dq_ref, dk_ref, dv_ref, dk_s, dv_s):
    cos, sin = cos_ref[...], -sin_ref[...]
    for at in reversed(range(0, T, BQ)):
        n, mine = at + BQ, slice(at, at + BQ)
        q, do = qr_ref[mine, :], do_ref[mine, :]
        delta = (wide(do) * wide(o_ref[mine, :])).T.sum(axis=0, keepdims=True)
        p = masked(jnp.exp2(dot(kr_ref[:n, :], q, 1, 1) * (SCALE * LOG2E) - lse_ref[0, :, mine]), n, 0.0)
        ds = low(p * (dot(v_ref[:n, :], do, 1, 1) - delta))
        dv, dk = dot(low(p), do, 1, 0), dot(ds, q, 1, 0)
        if n == T:
            dv_s[...], dk_s[...] = dv, dk
        else:
            dv_s[:n, :] += dv
            dk_s[:n, :] += dk
        dq = low(dot(ds, kr_ref[:n, :], 0, 0) * SCALE)
        dq_ref[mine, :] = low(turn(wide(dq), cos[mine], sin[mine]))
    dk_ref[...] = low(turn(wide(low(dk_s[...] * SCALE)), cos, sin))
    dv_ref[...] = low(dv_s[...])


HEAD_SPEC = pl.BlockSpec((T, HEAD), lambda h: (0, h))
TABLE = pl.BlockSpec((T, HEAD // 2), lambda h: (0, 0))
LSE = pl.BlockSpec((1, 1, T), lambda h: (h, 0, 0))
WHOLE = jax.ShapeDtypeStruct((T, D), bf16)


def attend(q, k, v, cos, sin):
    return pl.pallas_call(
        attend_kernel,
        grid=(D // HEAD,),
        in_specs=[HEAD_SPEC] * 3 + [TABLE] * 2,
        out_specs=[HEAD_SPEC] * 3 + [LSE],
        out_shape=[WHOLE] * 3 + [jax.ShapeDtypeStruct((D // HEAD, 1, T), f32)],
        cost_estimate=pl.CostEstimate(flops=3 * 2**30, transcendentals=2**21, bytes_accessed=2**24),
    )(q, k, v, cos, sin)


def attend_back(qr, kr, v, o, do, lse, cos, sin):
    return pl.pallas_call(
        attend_back_kernel,
        grid=(D // HEAD,),
        in_specs=[HEAD_SPEC] * 5 + [LSE] + [TABLE] * 2,
        out_specs=[HEAD_SPEC] * 3,
        out_shape=[WHOLE] * 3,
        scratch_shapes=[pltpu.VMEM((T, HEAD), f32)] * 2,
        cost_estimate=pl.CostEstimate(flops=7 * 2**30, transcendentals=2**21, bytes_accessed=2**24),
    )(qr, kr, v, o, do, lse, cos, sin)


MESH = pl.DeviceIdType.MESH
ROWS = (8, 8, 8, 8, 8, 8, 32)
COLS = (1024, 1024, 1024, 1024, 4096, 4096, 1024)


def place():
    me = lax.axis_index("dp")
    return [me // 32, (me // 8) % 4, (me // 2) % 4, me % 2]


def at(co):
    return {"dp": ((co[0] * 4 + co[1]) * 4 + co[2]) * 2 + co[3]}


def moved(co, axis, by):
    co = list(co)
    co[axis] = lax.rem(co[axis] + (by + 4), 4)
    return co


def remote(src, dst, send_sem, recv_sem, to):
    return pltpu.make_async_remote_copy(src, dst, send_sem, recv_sem, device_id=at(to), device_id_type=MESH)


def greet(peers):
    barrier = pltpu.get_barrier_semaphore()
    for p in peers:
        pl.semaphore_signal(barrier, inc=1, device_id=at(p), device_id_type=MESH)
    pl.semaphore_wait(barrier, len(peers))


TURNS = ((0, 1, 2), (1, 2, 0), (2, 0, 1))
GATHER = (
    ((0, 0, 1024, 0), (1, 0, 1024, 1), (2, 0, 1024, 2), (3, 0, 384, 0), (3, 384, 256, 1), (3, 640, 384, 2)),
    ((4, 0, 4096, 0), (5, 0, 4096, 1), (6, 0, 1024, 2)),
)


def gather_kernel(*refs):
    src, out = refs[:7], refs[7:14]
    lsem, ssem, rsem = refs[14:]
    co = place()
    other = co[:3] + [1 - co[3]]
    local = [pltpu.make_async_copy(src[m], out[m].at[co[0], co[1], co[2], co[3]], lsem.at[m]) for m in range(7)]
    for cp in local:
        cp.start()
    greet([moved(co, a, s) for a in range(3) for s in (1, 2, 3)] + [other])
    for cp in local:
        cp.wait()
    started = []

    def send(piece, sel, cols, to):
        i = len(started)
        ref = out[piece[0]].at[sel[0], sel[1], sel[2], co[3], :, pl.ds(cols[0], cols[1])]
        cp = remote(ref, ref, ssem.at[i], rsem.at[i], to)
        cp.start()
        started.append(cp)
        return cp

    def block(piece, phase, a):
        sel = list(co[:3])
        for k in range(phase):
            sel[TURNS[piece[3]][k]] = slice(None)
        sel[TURNS[piece[3]][phase]] = a
        return sel

    def run(g):
        pieces = GATHER[g]
        whole = lambda p: (p[1], p[2])
        for phase in (0, 1):
            got = []
            for p in pieces:
                ax = TURNS[p[3]][phase]
                got += [send(p, block(p, phase, co[ax]), whole(p), moved(co, ax, s)) for s in (1, 3, 2)]
            yield
            for cp in got:
                cp.wait_recv()
        got = []
        for p in pieces:
            ax = TURNS[p[3]][2]
            own = block(p, 2, co[ax])
            got.append([send(p, own, whole(p), moved(co, ax, s)) for s in (1, 3)])
        across = [send(p, block(p, 2, co[TURNS[p[3]][2]]), whole(p), other) for p in pieces]
        yield
        last = []
        for k, s in enumerate((1, 3)):
            for p, cps in zip(pieces, got):
                ax = TURNS[p[3]][2]
                cps[k].wait_recv()
                sel = block(p, 2, moved(co, ax, 4 - s)[ax])
                h = (p[2] // 256) * 128
                cols = (p[1], h) if s == 1 else (p[1] + h, p[2] - h)
                last.append((p, cols, s, send(p, sel, cols, moved(co, ax, s))))
                across.append(send(p, sel, whole(p), other))
        yield
        for p, cols, s, cp in last:
            ax = TURNS[p[3]][2]
            cp.wait_recv()
            across.append(send(p, block(p, 2, moved(co, ax, 2)[ax]), cols, other))
        yield
        for cp in across:
            cp.wait_recv()

    runs = [run(g) for g in range(len(GATHER))]
    alive = list(runs)
    while alive:
        for r in list(alive):
            if next(r, "end") == "end":
                alive.remove(r)
    for cp in started:
        cp.wait_send()


def gather(shards):
    n = sum(len(g) for g in GATHER) * 15
    outs = pl.pallas_call(
        gather_kernel,
        out_shape=[jax.ShapeDtypeStruct((4, 4, 4, 2, r, n), jnp.bfloat16) for r, n in zip(ROWS, COLS)],
        in_specs=[pl.BlockSpec(memory_space=pltpu.VMEM)] * 7,
        out_specs=[pl.BlockSpec(memory_space=pl.ANY)] * 7,
        scratch_shapes=[pltpu.SemaphoreType.DMA((7,)), pltpu.SemaphoreType.DMA((n,)), pltpu.SemaphoreType.DMA((n,))],
        compiler_params=pltpu.CompilerParams(collective_id=0, has_side_effects=True),
    )(*shards)
    return [o.reshape(128 * r, n) for o, r, n in zip(outs, ROWS, COLS)]

U_ORD = {"x": (0, 2, 1), "y": (1, 0, 2), "z": (2, 1, 0)}
GROUPS = [[(4, 1024 * j, "g", "x"), (5, 1024 * j, "g", "y"), (6, j, "d", "z")] for j in range(4)] + \
         [[(0, 0, "g", "x"), (1, 0, "g", "y"), (2, 0, "g", "z"), (3, 0, "g", "x")]]

def rs_kernel(*refs):
    src, outs = refs[:7], refs[7:14]
    own, rd, r1, r2, r3, s1, s2, s2d, rx, lsem, dsem, s1sem, s2sem, s3sem, xsem = refs[14:]
    co = place()
    c = co[3]
    other = co[:3] + [1 - c]
    peers = [moved(co, a, s) for a in range(3) for s in (1, 2, 3)] + [other]
    bar = pltpu.get_barrier_semaphore()
    for p in peers:
        pl.semaphore_signal(bar, inc=1, device_id=at(p), device_id_type=MESH)
    pl.semaphore_wait(bar, len(peers))

    def srcsel(u, core):
        m, k, kind, o = u
        return src[m].at[:, :, :, core, :, pl.ds(k, 1024)] if kind == "g" else src[m].at[k, :, :, core]

    def view(ref, kind):
        return ref if kind == "g" else ref.reshape(4, 4, 32, 1024)

    def start0(g):
        cps = []
        for i, u in enumerate(GROUPS[g]):
            p = g % 2
            l = pltpu.make_async_copy(srcsel(u, c), view(own.at[p, i], u[2]), lsem.at[p, i])
            l.start()
            d = remote(srcsel(u, 1 - c), view(rd.at[p, i], u[2]), dsem.at[0, p, i], dsem.at[1, p, i], other)
            d.start()
            cps.append((l, d))
        return cps

    def at_dim(ref, d, a):
        ix = [slice(None)] * d + [a]
        return ref.at[tuple(ix)]

    def axes_of(u):
        o = U_ORD[u[3]]
        if u[2] == "g":
            dims, left = [], [0, 1, 2]
            for a in o:
                dims.append((a, left.index(a))); left.remove(a)
            return dims
        return [(2, 1), (1, 0)]

    def sends(ref, buf, sem, ax, dim, p, i):
        out = []
        for s in (1, 2, 3):
            to = moved(co, ax, s)
            cp = remote(at_dim(ref, dim, to[ax]), buf.at[p, i, s - 1], sem.at[0, p, i, s - 1], sem.at[1, p, i, s - 1], to)
            cp.start(); out.append(cp)
        return out

    f32 = lambda v: v.astype(jnp.float32)
    state = {}

    def stage1(g):
        p = g % 2
        res = []
        for i, u in enumerate(GROUPS[g]):
            l, d = state[g, 0][i]
            l.wait(); d.wait_recv()
            for x in range(4):
                def add(k, _, x=x):
                    own[p, i, x, k] = (f32(own[p, i, x, k]) + f32(rd[p, i, x, k])).astype(jnp.bfloat16); return 0
                lax.fori_loop(0, 4, add, 0)
            ax, dim = axes_of(u)[0]
            res.append(sends(own.at[p, i], r1, s1sem, ax, dim, p, i))
        return res

    def stage2(g):
        p = g % 2
        res = []
        for i, u in enumerate(GROUPS[g]):
            for cp in state[g, 1][i]: cp.wait()
            state[g, 0][i][1].wait_send()
            ax, dim = axes_of(u)[0]
            mine = at_dim(own.at[p, i], dim, co[ax])
            for k in range(4):
                v = f32(mine[k]) + f32(r1[p, i, 0, k]) + f32(r1[p, i, 1, k]) + f32(r1[p, i, 2, k])
                s1[p, i, k] = v.astype(jnp.bfloat16)
            ax, dim = axes_of(u)[1]
            res.append(sends(s1.at[p, i], r2, s2sem, ax, dim, p, i))
        return res

    def stage3(g):
        p = g % 2
        res = []
        for i, u in enumerate(GROUPS[g]):
            for cp in state[g, 2][i]: cp.wait()
            ax, dim = axes_of(u)[1]
            mine = at_dim(s1.at[p, i], dim, co[ax])
            v = f32(mine[...]) + f32(r2[p, i, 0]) + f32(r2[p, i, 1]) + f32(r2[p, i, 2])
            if u[2] == "d":
                s2d[u[1]] = v.astype(jnp.bfloat16)
                res.append([])
            else:
                s2[p, i] = v.astype(jnp.bfloat16)
                ax, dim = axes_of(u)[2]
                res.append(sends(s2.at[p, i], r3, s3sem, ax, dim, p, i))
        return res

    def stage4(g):
        p = g % 2
        for i, u in enumerate(GROUPS[g]):
            if u[2] == "g":
                for cp in state[g, 3][i]: cp.wait()
                ax, dim = axes_of(u)[2]
                mine = at_dim(s2.at[p, i], dim, co[ax])
                v = f32(mine[...]) + f32(r3[p, i, 0]) + f32(r3[p, i, 1]) + f32(r3[p, i, 2])
                outs[u[0]][:, pl.ds(u[1], 1024)] = v.astype(jnp.bfloat16)

    stages = [start0, stage1, stage2, stage3, stage4]
    n = len(GROUPS)
    for t in range(n + 4):
        for s in (4, 3, 2, 1, 0):
            g = t - s
            if 0 <= g < n:
                state[g, s] = stages[s](g)
        if t == 6:
            xs = []
            for s in (1, 2, 3):
                to = moved(co, 0, s)
                cp = remote(s2d.at[to[0]], rx.at[s - 1], xsem.at[0, s - 1], xsem.at[1, s - 1], to)
                cp.start(); xs.append(cp)
    for cp in xs: cp.wait()
    v = f32(s2d[co[0]]) + f32(rx[0]) + f32(rx[1]) + f32(rx[2])
    outs[6][...] = v.astype(jnp.bfloat16).reshape(32, 1024)

def rs_call(dws):
    bf = jnp.bfloat16
    V = pltpu.VMEM; D = pltpu.SemaphoreType.DMA
    return pl.pallas_call(
        rs_kernel,
        out_shape=[jax.ShapeDtypeStruct((r, n), bf) for r, n in zip(ROWS, COLS)],
        in_specs=[pl.BlockSpec(memory_space=pl.ANY)] * 7,
        out_specs=[pl.BlockSpec(memory_space=pltpu.VMEM)] * 7,
        scratch_shapes=[V((2, 4, 4, 4, 4, 8, 1024), bf), V((2, 4, 4, 4, 4, 8, 1024), bf), V((2, 4, 3, 4, 4, 8, 1024), bf), V((2, 4, 3, 4, 8, 1024), bf),
                        V((2, 4, 3, 8, 1024), bf), V((2, 4, 4, 4, 8, 1024), bf), V((2, 4, 4, 8, 1024), bf), V((4, 4, 8, 1024), bf), V((3, 4, 8, 1024), bf),
                        D((2, 4)), D((2, 2, 4)), D((2, 2, 4, 3)), D((2, 2, 4, 3)), D((2, 2, 4, 3)), D((2, 3))],
        compiler_params=pltpu.CompilerParams(collective_id=1, has_side_effects=True, vmem_limit_bytes=60 * 2**20),
    )(*[w.reshape(4, 4, 4, 2, r, n) for w, r, n in zip(dws, ROWS, COLS)])


def matmul(a, w, ca=1, cb=0):
    return low(dot(a, w, ca, cb))


def normed(h):
    scale = lax.rsqrt(jnp.mean(wide(h) ** 2, -1, keepdims=True) + EPS)
    return low(wide(h) * scale), scale


def normed_back(h, scale, by_out):
    by_out, h = wide(by_out), wide(h)
    return low(by_out * scale - h * (scale**3 * jnp.mean(by_out * h, -1, keepdims=True)))


def solution(mesh):
    def step(x, dy, *weights):
        wq, wk, wv, wo, wg, wu, wd = gather([w[0] for w in weights])
        x, dy = x[0], dy[0]
        half = HEAD // 2
        angle = jnp.arange(T, dtype=f32)[:, None] * THETA ** (-jnp.arange(half, dtype=f32) / half)
        cos, sin = jnp.cos(angle), jnp.sin(angle)
        a, scale_a = normed(x)
        v = matmul(a, wv)
        o, qr, kr, lse = attend(matmul(a, wq), matmul(a, wk), v, cos, sin)
        h = x + matmul(o, wo)
        b, scale_b = normed(h)
        gate, up = dot(b, wg, 1, 0), dot(b, wu, 1, 0)
        s = jax.nn.sigmoid(gate)
        by_act = wide(matmul(dy, wd, 1, 1))
        by_wd = matmul(low(gate * s * up), dy, 0, 0)
        by_gate, by_up = low(by_act * up * (s * (1 + gate * (1 - s)))), low(by_act * (gate * s))
        by_wg, by_wu = matmul(b, by_gate, 0, 0), matmul(b, by_up, 0, 0)
        by_b = matmul(by_gate, wg, 1, 1) + matmul(by_up, wu, 1, 1)
        by_h = dy + normed_back(h, scale_b, by_b)
        by_wo = matmul(o, by_h, 0, 0)
        by_q, by_k, by_v = attend_back(qr, kr, v, o, matmul(by_h, wo, 1, 1), lse, cos, sin)
        by_w = [matmul(a, g, 0, 0) for g in (by_q, by_k, by_v)] + [by_wo, by_wg, by_wu, by_wd]
        by_a = matmul(by_q, wq, 1, 1) + matmul(by_k, wk, 1, 1) + matmul(by_v, wv, 1, 1)
        by_x = by_h + normed_back(x, scale_a, by_a)
        return (by_x[None], *(m[None] for m in rs_call(by_w)))

    states, cut = P(("rep", "dp"), None, None), P(None, "dp", None)
    return jax.shard_map(
        step,
        mesh=mesh,
        in_specs=(states, states) + (cut,) * 7,
        out_specs=(states,) + (P("rep", "dp", None),) * 7,
        check_vma=False,
    )
```
